128 devices in a mesh: dom: 128 (over y, z, x, core).
Axes of the slice: x: 4, y: 4, z: 4, core: 2. Of those that a mesh axis runs over, the one named last changes fastest.
Arguments:
- features: bfloat16 [65536, 512], P('dom'), may hold values from -6 to 6
- weights: bfloat16 [3, 512, 512], replicated, may hold values from -0.078125 to 0.078125
- halo_send: int32 [128, 128, 4], P('dom'), may hold values from 0 to 511
- nbr_index: int32 [65536, 2, 8], P('dom'), may hold values from 0 to 1023
- tile_count: int32 [128], P('dom'), may hold values from 1 to 16, as said below
- edge_ends: int32 [2048, 2, 256], P('dom'), may hold values from 0 to 511
- neg_ids: int32 [1024], P('dom'), may hold values from 0 to 511
Outputs:
- weight_grad: float32 [3, 512, 512], replicated
- mean_loss: float32 [], replicated
- pre_grad: bfloat16 [65536, 512], P('dom')
The draws below stay inside these ranges and needn't reach their ends.
Inputs may be any that keep to these rules, and one draw needn't show every extreme that they name: `nbr_index`: an entry below 512 names a row of the node's own partition; an entry 512 + q * 4 + k names slot k of the halo from partition q. `tile_count`: partition 128 - 1 holds 16 tiles; every other partition holds at most 8. `edge_ends`: tile slots at or past a partition's tile_count hold no edges. `neg_ids`: entry j names a row of partition j // 8.
All inputs are finite; a program needn't handle non-finite values.
Results may differ from the reference program's by a relative error of at most 0.0012.
The reference program's roundings to bfloat16 on the way count: a program that leaves them out, or rounds other values in their place, can miss the bound.
Values may be sent and summed in bfloat16 or wider, within the bound.
A program may use at most 64 MiB of HBM per device.

```python
import jax
import jax.numpy as jnp
from jax import lax

H = 512
RELS = 2
FAN = 8
TILE = 256
NODE_DEV = 512
HALO_PEER = 4
MAX_TILES = 16
NEG_DEV = 8
NODES = 65536
NEG = 1024
SLOTS = 1024
N_DOM = 128


def draw_tile_count(key, part):
    first = jax.random.randint(jax.random.fold_in(key, 11), (N_DOM,), 0, MAX_TILES)
    second = jax.random.randint(jax.random.fold_in(key, 12), (N_DOM,), 0, MAX_TILES)
    counts = 1 + first * second // (2 * MAX_TILES)
    return jnp.where(jnp.arange(N_DOM) == N_DOM - 1, MAX_TILES, counts).astype(jnp.int32)


def touch_ends(values, own_key, low, top_value):
    longest = values.shape.index(max(values.shape))
    spots = []
    for shift in (0, 1):
        where = [jax.random.randint(jax.random.fold_in(own_key, axis), (), 0, length) for axis, length in enumerate(values.shape)]
        where[longest] = (where[longest] + shift) % values.shape[longest]
        spots.append(tuple(where))
    return values.at[spots[0]].set(low).at[spots[1]].set(top_value)


def levels(key, dims, split, low, largest):
    def one(axis_at, blocks):
        steps = jax.random.uniform(jax.random.fold_in(jax.random.fold_in(key, 6), axis_at), (blocks,), jnp.float32, low / len(split), largest / len(split))
        return jnp.repeat(jnp.exp(steps), dims[axis_at] // blocks).reshape((-1,) + (1,) * (len(dims) - axis_at - 1))

    factor_of = one(*split[0])
    for cut in split[1:]:
        factor_of = factor_of * one(*cut)
    return factor_of


def centred(key, extent, scale, limit, split=(), kind=jnp.bfloat16):
    entries = jax.random.normal(key, extent, jnp.float32) * scale
    if len(split) > 0:
        entries = levels(key, extent, split, -0.22, 0.18) * entries
    return jnp.clip(entries, min=-limit, max=limit).astype(kind)


def setup_inputs(seed: int = 0) -> dict:
    seeds = jax.random.split(jax.random.key(seed), 8)
    return {
        "features": centred(seeds[0], (NODES, H), 1.0, 6.0, ((0, 128),)),
        "weights": centred(seeds[1], (RELS + 1, H, H), (12 * H) ** -0.5, 0.078125),
        "halo_send": touch_ends(jax.random.randint(seeds[2], (N_DOM, N_DOM, HALO_PEER), 0, NODE_DEV), jax.random.fold_in(seeds[2], 1), 0, NODE_DEV - 1).astype(jnp.int32),
        "nbr_index": touch_ends(jax.random.randint(seeds[3], (NODES, RELS, FAN), 0, SLOTS), jax.random.fold_in(seeds[3], 1), 0, SLOTS - 1).astype(jnp.int32),
        "tile_count": draw_tile_count(jax.random.fold_in(seeds[7], 71), 0),
        "edge_ends": touch_ends(jax.random.randint(seeds[5], (N_DOM * MAX_TILES, 2, TILE), 0, NODE_DEV), jax.random.fold_in(seeds[5], 1), 0, NODE_DEV - 1).astype(jnp.int32),
        "neg_ids": touch_ends(jax.random.randint(seeds[6], (NEG,), 0, NODE_DEV), jax.random.fold_in(seeds[6], 1), 0, NODE_DEV - 1).astype(jnp.int32),
    }


def neighbour_mean(lookup, neighbours):
    running_sum = jnp.zeros((neighbours.shape[0], lookup.shape[1]), jnp.float32)
    for column in range(neighbours.shape[1]):
        running_sum = running_sum + lookup[neighbours[:, column]].astype(jnp.float32)
    return (running_sum / neighbours.shape[1]).astype(jnp.bfloat16)


def score_tile(source, target, negatives):
    source_wide = source.astype(jnp.float32)
    target_wide = target.astype(jnp.float32)
    positive = jnp.sum(source_wide * target_wide, axis=1)
    negative = lax.dot_general(source, negatives, (((1,), (1,)), ((), ())), preferred_element_type=jnp.float32)
    count_neg = negatives.shape[0]
    tile_loss = jnp.sum(jnp.logaddexp(0.0, -positive)) + jnp.sum(jnp.logaddexp(0.0, negative)) / count_neg
    grad_positive = -jax.nn.sigmoid(-positive)
    grad_negative = (jax.nn.sigmoid(negative) / count_neg).astype(jnp.bfloat16)
    source_grad = grad_positive[:, None] * target_wide + jnp.dot(grad_negative, negatives, preferred_element_type=jnp.float32)
    target_grad = grad_positive[:, None] * source_wide
    negative_grad = lax.dot_general(grad_negative, source, (((0,), (0,)), ((), ())), preferred_element_type=jnp.float32)
    return tile_loss, source_grad, target_grad, negative_grad


def reference(features, weights, halo_send, nbr_index, tile_count, edge_ends, neg_ids):
    def layer_part(partition):
        own_rows = lax.dynamic_slice_in_dim(features, partition * NODE_DEV, NODE_DEV, 0)
        sender = jnp.arange(N_DOM, dtype=jnp.int32)[:, None] * NODE_DEV
        halo_index = (sender + halo_send[:, partition, :]).reshape(-1).astype(jnp.int32)
        lookup = jnp.concatenate([own_rows, features[halo_index]], 0)
        neighbours = lax.dynamic_slice_in_dim(nbr_index, partition * NODE_DEV, NODE_DEV, 0)
        preact = jnp.dot(own_rows, weights[0], preferred_element_type=jnp.float32)
        means = []
        for relation in range(RELS):
            mean_rows = neighbour_mean(lookup, neighbours[:, relation, :])
            means.append(mean_rows)
            preact = preact + jnp.dot(mean_rows, weights[relation + 1], preferred_element_type=jnp.float32)
        return preact, jnp.stack(means)

    parts = jnp.arange(N_DOM, dtype=jnp.int32)
    preact, means = lax.map(layer_part, parts)
    embedding = preact.astype(jnp.bfloat16)
    flat_rows = embedding.reshape(-1, H)
    neg_rows = (jnp.arange(NEG, dtype=jnp.int32) // NEG_DEV) * NODE_DEV + neg_ids
    negatives = flat_rows[neg_rows]

    def per_part(state_now, partition):
        loss_sum, negative_total = state_now
        own_embed = embedding[partition]
        tile_ends = lax.dynamic_slice_in_dim(edge_ends, partition * MAX_TILES, MAX_TILES, 0)

        def tile_step(tile_index, running):
            tile_loss_sum, node_grad, neg_grad = running
            pair_ends = lax.dynamic_index_in_dim(tile_ends, tile_index, 0, keepdims=False)
            tile_loss, source_grad, target_grad, negative_grad = score_tile(own_embed[pair_ends[0]], own_embed[pair_ends[1]], negatives)
            node_grad = node_grad.at[pair_ends[0]].add(source_grad).at[pair_ends[1]].add(target_grad)
            return tile_loss_sum + tile_loss, node_grad, neg_grad + negative_grad

        initial = (jnp.zeros((), jnp.float32), jnp.zeros((NODE_DEV, H), jnp.float32), negative_total)
        tile_loss_sum, node_grad, negative_total = lax.fori_loop(0, tile_count[partition], tile_step, initial)
        return (loss_sum + tile_loss_sum, negative_total), node_grad

    start_state = (jnp.zeros((), jnp.float32), jnp.zeros((NEG, H), jnp.float32))
    (loss_sum, negative_total), node_grad = lax.scan(per_part, start_state, parts)
    node_grad = node_grad.reshape(-1, H).at[neg_rows].add(negative_total).reshape(N_DOM, NODE_DEV, H)
    pre_grad = node_grad.astype(jnp.bfloat16)
    feature_parts = features.reshape(N_DOM, NODE_DEV, H)

    def grad_part(running, items):
        own_rows, mean_rows, grad_rows = items
        terms = [lax.dot_general(own_rows, grad_rows, (((0,), (0,)), ((), ())), preferred_element_type=jnp.float32)]
        for relation in range(RELS):
            terms.append(lax.dot_general(mean_rows[relation], grad_rows, (((0,), (0,)), ((), ())), preferred_element_type=jnp.float32))
        return running + jnp.stack(terms), None

    weight_sum, unused = lax.scan(grad_part, jnp.zeros((RELS + 1, H, H), jnp.float32), (feature_parts, means, pre_grad))
    edge_total = jnp.sum(tile_count).astype(jnp.float32) * TILE
    return weight_sum / edge_total, loss_sum / edge_total, pre_grad.reshape(-1, H)
```

```python
import jax
import jax.numpy as jnp
from jax import lax
from jax.experimental import pallas as pl
from jax.experimental.pallas import tpu as pltpu
from jax.sharding import PartitionSpec as P

MESH = pl.DeviceIdType.MESH
F32 = jnp.float32
BF16 = jnp.bfloat16
STRIDES = (32, 8, 2)


def nn(a, b):
    return lax.dot_general(a, b, (((1,), (0,)), ((), ())), preferred_element_type=F32)


def nt(a, b):
    return lax.dot_general(a, b, (((1,), (1,)), ((), ())), preferred_element_type=F32)


def tn(a, b):
    return lax.dot_general(a, b, (((0,), (0,)), ((), ())), preferred_element_type=F32)


def split(x):
    hi = x.astype(BF16)
    lo = (x - hi.astype(F32)).astype(BF16)
    return hi, lo


def flat(block):
    wide = block.astype(F32)
    return wide.reshape(-1, wide.shape[-1]).astype(BF16)


def kernel(
    count_ref,
    ids_ref,
    feat_ref,
    wts_ref,
    halo_ref,
    nbr_ref,
    ends_ref,
    wout_ref,
    stat_ref,
    pre_ref,
    out_buf,
    in_buf,
    sel_ref,
    mean_ref,
    emb_ref,
    one_a,
    one_b,
    pair_ref,
    sym_ref,
    dotp_ref,
    hi_ref,
    lo_ref,
    neg_blk,
    neg_buf,
    score_ref,
    gneg_ref,
    grad_ref,
    wide_ref,
    sib_out,
    sib_in,
    rs_out,
    rs_in,
    part_ref,
    wsib_ref,
    s1_ref,
    s2_ref,
    s3_ref,
    a1_ref,
    a2_ref,
    a3_ref,
    t_out,
    t_in,
    ex_send,
    ex_recv,
    sib_send,
    sib_recv,
    w_send,
    w_recv,
    t_send,
    t_recv,
):
    me = lax.axis_index("dom")
    chip, core = me // 2, me % 2
    other = 1 - core
    sibling = me + 1 - 2 * core
    coords = (chip // 16, (chip // 4) % 4, chip % 4)
    barrier = pltpu.get_barrier_semaphore()

    def hello(s, carry):
        pl.semaphore_signal(
            barrier, inc=1, device_id=((me + s) % 128,), device_id_type=MESH
        )
        return carry

    lax.fori_loop(1, 128, hello, 0)

    def remote(src, dst, send, recv, to):
        return pltpu.make_async_remote_copy(
            src_ref=src,
            dst_ref=dst,
            send_sem=send,
            recv_sem=recv,
            device_id=(to,),
            device_id_type=MESH,
        )

    def spread(src_of, dst, phase):
        def body(s, carry):
            to = (chip + s) % 64
            remote(
                src_of(to), dst, ex_send.at[phase], ex_recv.at[phase], 2 * to + core
            ).start()
            return carry

        lax.fori_loop(1, 64, body, 0)

    def arrived(buf, phase):
        whole = buf.at[pl.ds(0, 63)]
        remote(whole, whole, ex_send.at[phase], ex_recv.at[phase], sibling).wait_recv()

    def left(buf, phase):
        whole = buf.at[pl.ds(0, 63)]
        remote(whole, whole, ex_send.at[phase], ex_recv.at[phase], sibling).wait_send()

    halo_ids = halo_ref[...]
    pick = jnp.where(
        lax.broadcasted_iota(jnp.int32, (512, 512), 0) == halo_ids, 1.0, 0.0
    ).astype(BF16)
    out_buf[...] = tn(pick, feat_ref[...]).reshape(64, 8, 512).astype(BF16)
    in_buf[core, chip] = out_buf[chip]

    pl.semaphore_wait(barrier, 127)
    spread(lambda to: out_buf.at[to], in_buf.at[core, chip], 0)

    count = count_ref[0]
    live = lax.broadcasted_iota(jnp.int32, (16, 256), 0) < count
    pair_ref[...] = jnp.zeros_like(pair_ref)

    def add_tiles(group, carry):
        for t in range(4):
            tile = group * 4 + t
            row = ends_ref[pl.ds(tile, 1), :]
            used = lax.broadcasted_iota(jnp.int32, (1, 256), 0) + tile < count
            source = jnp.where(used, row[:, :256], -1)
            target = row[:, 256:]
            for h in range(4):
                nodes = lax.broadcasted_iota(jnp.int32, (128, 256), 0) + h * 128
                at = (slice(h * 128, h * 128 + 128), slice(t * 256, t * 256 + 256))
                one_a[at] = jnp.where(nodes == source, 1.0, 0.0).astype(BF16)
                one_b[at] = jnp.where(nodes == target, 1.0, 0.0).astype(BF16)
        pair_ref[...] += nt(one_a[...], one_b[...])
        return carry

    lax.fori_loop(0, 4, add_tiles, 0)
    sym_ref[...] = pair_ref[...] + pair_ref[...].T

    def count_rows(step, carry):
        rows = pl.ds(pl.multiple_of(step * 32, 32), 32)
        ids = nbr_ref[rows, :]
        past = ids - 512
        slot = (
            512
            + ((past // 4) % 2) * 512
            + (past // 8) * 8
            + core * 4
            + past % 4
        )
        ids = jnp.where(ids < 512, ids, slot)
        for r in range(2):
            for part in range(3):
                lanes = lax.broadcasted_iota(jnp.int32, (32, 512), 1) + part * 512
                total = jnp.zeros((32, 512), F32)
                for j in range(8):
                    col = ids[:, r * 8 + j : r * 8 + j + 1]
                    total = total + jnp.where(lanes == col, 1.0, 0.0)
                sel_ref[r, rows, part * 512 : part * 512 + 512] = total.astype(BF16)
        return carry

    lax.fori_loop(0, 16, count_rows, 0)

    arrived(in_buf.at[core], 0)
    to_sib = remote(
        in_buf.at[core], in_buf.at[core], sib_send.at[0], sib_recv.at[0], sibling
    )
    to_sib.start()
    preact = nn(feat_ref[...], wts_ref[0])
    to_sib.wait()
    left(out_buf, 0)

    table = flat(in_buf[...].reshape(1024, 512))
    for r in range(2):
        total = nn(sel_ref[r, :, :512], feat_ref[...]) + nn(sel_ref[r, :, 512:], table)
        mean = (total * 0.125).astype(BF16)
        mean_ref[r] = mean
        preact = preact + nn(mean, wts_ref[r + 1])
    emb_ref[...] = preact.astype(BF16)

    row_of = lax.broadcasted_iota(jnp.int32, (8, 512), 0)
    named = jnp.zeros((8, 512), jnp.int32)
    for j in range(8):
        named = jnp.where(row_of == j, ids_ref[j], named)
    pick_neg = jnp.where(
        named == lax.broadcasted_iota(jnp.int32, (8, 512), 1), 1.0, 0.0
    ).astype(BF16)
    own_neg = nn(pick_neg, emb_ref[...]).astype(BF16)
    neg_blk[...] = own_neg
    neg_buf[core, chip] = own_neg
    spread(lambda to: neg_blk, neg_buf.at[core, chip], 1)

    dotp_ref[...] = nt(emb_ref[...], emb_ref[...])

    def positive_rows(step, loss):
        rows = pl.ds(pl.multiple_of(step * 32, 32), 32)
        dots, weight = dotp_ref[rows, :], sym_ref[rows, :]
        small = jnp.exp(-jnp.abs(dots))
        below = jnp.where(dots >= 0, small, 1.0) / (1.0 + small)
        loss = loss + weight * (jnp.maximum(-dots, 0.0) + jnp.log1p(small))
        hi, lo = split(-weight * below)
        hi_ref[rows, :] = hi
        lo_ref[rows, :] = lo
        return loss

    loss_pos = lax.fori_loop(0, 16, positive_rows, jnp.zeros((32, 512), F32))
    emb = emb_ref[...]
    grad_ref[...] = nn(hi_ref[...], emb) + nn(lo_ref[...], emb)
    degree = jnp.sum(pair_ref[...], axis=1, keepdims=True)
    hi, lo = split(emb.astype(F32) * degree)
    hi_ref[...] = hi
    lo_ref[...] = lo

    arrived(neg_buf.at[core], 1)
    to_sib = remote(
        neg_buf.at[core], neg_buf.at[core], sib_send.at[1], sib_recv.at[1], sibling
    )
    to_sib.start()
    to_sib.wait()
    whole = neg_buf.at[core].at[pl.ds(0, 63)]
    remote(whole, whole, ex_send.at[1], ex_recv.at[1], sibling).wait_send()

    negs = flat(neg_buf[...].reshape(1024, 512))
    score_ref[...] = nt(emb_ref[...], negs)

    def negative_rows(step, loss):
        rows = pl.ds(pl.multiple_of(step * 16, 16), 16)
        dots = score_ref[rows, :]
        small = jnp.exp(-jnp.abs(dots))
        above = jnp.where(dots >= 0, 1.0, small) / (1.0 + small)
        gneg_ref[rows, :] = (above * (1.0 / 1024)).astype(BF16)
        soft = jnp.maximum(dots, 0.0) + jnp.log1p(small)
        many = jnp.sum(pair_ref[rows, :], axis=1, keepdims=True)
        return loss + soft * many

    loss_neg = lax.fori_loop(0, 32, negative_rows, jnp.zeros((16, 1024), F32))
    wide = tn(gneg_ref[...], hi_ref[...]) + tn(gneg_ref[...], lo_ref[...])
    wide_ref[...] = wide.reshape(2, 64, 8, 512)
    sib_out[...] = wide_ref[other].astype(BF16)
    to_sib = remote(sib_out, sib_in, sib_send.at[2], sib_recv.at[2], sibling)
    to_sib.start()
    grad_ref[...] += degree * nn(gneg_ref[...], negs)
    to_sib.wait()
    rs_out[...] = (wide_ref[core] + sib_in[...].astype(F32)).astype(BF16)
    rs_in[chip] = rs_out[chip]
    spread(lambda to: rs_out.at[to], rs_in.at[chip], 2)

    loss = 0.5 * jnp.sum(loss_pos) + jnp.sum(loss_neg) * (1.0 / 1024)
    lane = lax.broadcasted_iota(jnp.int32, (8, 128), 1)
    total = jnp.where(
        lane == 0, loss, jnp.where(lane == 1, count.astype(F32) * 256.0, 0.0)
    )

    arrived(rs_in, 2)
    left(rs_out, 2)
    neg_total = jnp.sum(rs_in[...].astype(F32), axis=0)
    hi, lo = split(neg_total)
    row_at = lax.broadcasted_iota(jnp.int32, (512, 8), 0)
    lane_at = lax.broadcasted_iota(jnp.int32, (512, 8), 1)
    named = jnp.zeros((512, 8), jnp.int32)
    for j in range(8):
        named = jnp.where(lane_at == j, ids_ref[j], named)
    put = jnp.where(named == row_at, 1.0, 0.0).astype(BF16)
    pre = (grad_ref[...] + nn(put, hi) + nn(put, lo)).astype(BF16)
    pre_ref[...] = pre

    half = pl.ds(pl.multiple_of(core * 256, 256), 256)
    other_half = pl.ds(pl.multiple_of(other * 256, 256), 256)
    sends = []
    for r in range(3):
        x = feat_ref[...] if r == 0 else mean_ref[r - 1]
        part_ref[r] = tn(x, pre)
        c = remote(
            part_ref.at[r, other_half],
            wsib_ref.at[r],
            w_send.at[6, r],
            w_recv.at[6, r],
            sibling,
        )
        c.start()
        sends.append(c)
    t_out[0] = total
    c = remote(t_out.at[0], t_in.at[3, 0], t_send.at[3], t_recv.at[3], sibling)
    c.start()
    sends.append(c)
    for c in sends:
        c.wait()
    total = total + t_in[3, 0]
    for r in range(3):
        part_ref[r, half, :] += wsib_ref[r]

    def peers(axis):
        mine, stride = coords[axis], STRIDES[axis]
        found = []
        for s in range(1, 4):
            q = (mine + s) % 4
            found.append((q, me + (q - mine) * stride))
        return mine, found

    def settle(buf, sems, i, j):
        whole = buf.at[pl.ds(0, 3)]
        remote(whole, whole, sems[0].at[i, j], sems[1].at[i, j], sibling).wait()

    landing = (s1_ref, s2_ref, s3_ref)
    for stage in range(3):
        t_out[stage + 1] = total
        for r in range(3):
            mine, found = peers((r + stage) % 3)
            for q, to in found:
                if stage == 0:
                    start = pl.multiple_of(core * 256 + q * 64, 64)
                    src = part_ref.at[r, pl.ds(start, 64)]
                elif stage == 1:
                    src = a1_ref.at[r, pl.ds(pl.multiple_of(q * 16, 16), 16)]
                else:
                    src = a2_ref.at[r, :, pl.ds(pl.multiple_of(q * 128, 128), 128)]
                slot = (mine - q + 4) % 4 - 1
                remote(
                    src,
                    landing[stage].at[r, slot],
                    w_send.at[stage, r],
                    w_recv.at[stage, r],
                    to,
                ).start()
        mine, found = peers(stage)
        for q, to in found:
            slot = (mine - q + 4) % 4 - 1
            remote(
                t_out.at[stage + 1],
                t_in.at[stage, slot],
                t_send.at[stage],
                t_recv.at[stage],
                to,
            ).start()
        for r in range(3):
            mine = coords[(r + stage) % 3]
            settle(landing[stage].at[r], (w_send, w_recv), stage, r)
            got = landing[stage][r]
            got = got[0] + got[1] + got[2]
            if stage == 0:
                start = pl.multiple_of(core * 256 + mine * 64, 64)
                a1_ref[r] = part_ref[r, pl.ds(start, 64), :] + got
            elif stage == 1:
                rows = pl.ds(pl.multiple_of(mine * 16, 16), 16)
                a2_ref[r] = a1_ref[r, rows, :] + got
            else:
                lanes = pl.ds(pl.multiple_of(mine * 128, 128), 128)
                a3_ref[r] = a2_ref[r, :, lanes] + got
        whole = t_in.at[stage]
        remote(whole, whole, t_send.at[stage], t_recv.at[stage], sibling).wait()
        total = total + t_in[stage, 0] + t_in[stage, 1] + t_in[stage, 2]

    edges = total[:, 1:2]
    stat_ref[...] = total / edges
    inverse = jnp.sum(jnp.where(lane == 1, total, 0.0)) * 0.125
    for stage in (2, 1, 0):
        for r in range(3):
            q1, q2, q3 = (coords[(r + s) % 3] for s in range(3))
            if stage == 2:
                start = pl.multiple_of(core * 256 + q1 * 64 + q2 * 16, 16)
                spot = (pl.ds(start, 16), pl.ds(pl.multiple_of(q3 * 128, 128), 128))
                wout_ref[r, spot[0], spot[1]] = a3_ref[r] / inverse
            elif stage == 1:
                start = pl.multiple_of(core * 256 + q1 * 64 + q2 * 16, 16)
                spot = (pl.ds(start, 16), slice(None))
            else:
                start = pl.multiple_of(core * 256 + q1 * 64, 64)
                spot = (pl.ds(start, 64), slice(None))
            block = wout_ref.at[r, spot[0], spot[1]]
            mine, found = peers((r + stage) % 3)
            for q, to in found:
                remote(
                    block, block, w_send.at[3 + stage, r], w_recv.at[3 + stage, r], to
                ).start()
        for r in range(3):
            settle(landing[stage].at[r], (w_send, w_recv), 3 + stage, r)
    sends = []
    for r in range(3):
        block = wout_ref.at[r, half]
        c = remote(block, block, w_send.at[7, r], w_recv.at[7, r], sibling)
        c.start()
        sends.append(c)
    for c in sends:
        c.wait()


def on_device(features, weights, halo_send, nbr_index, tile_count, edge_ends, neg_ids):
    vmem = pl.BlockSpec(memory_space=pltpu.VMEM)
    smem = pl.BlockSpec(memory_space=pltpu.SMEM)
    dma = pltpu.SemaphoreType.DMA
    wout, stat, pre = pl.pallas_call(
        kernel,
        out_shape=(
            jax.ShapeDtypeStruct((3, 512, 512), F32),
            jax.ShapeDtypeStruct((8, 128), F32),
            jax.ShapeDtypeStruct((512, 512), BF16),
        ),
        in_specs=[smem, smem] + [vmem] * 5,
        out_specs=(vmem, vmem, vmem),
        scratch_shapes=[
            pltpu.VMEM((64, 8, 512), BF16),
            pltpu.VMEM((2, 64, 8, 512), BF16),
            pltpu.VMEM((2, 512, 1536), BF16),
            pltpu.VMEM((2, 512, 512), BF16),
            pltpu.VMEM((512, 512), BF16),
            pltpu.VMEM((512, 1024), BF16),
            pltpu.VMEM((512, 1024), BF16),
            pltpu.VMEM((512, 512), F32),
            pltpu.VMEM((512, 512), F32),
            pltpu.VMEM((512, 512), F32),
            pltpu.VMEM((512, 512), BF16),
            pltpu.VMEM((512, 512), BF16),
            pltpu.VMEM((8, 512), BF16),
            pltpu.VMEM((2, 64, 8, 512), BF16),
            pltpu.VMEM((512, 1024), F32),
            pltpu.VMEM((512, 1024), BF16),
            pltpu.VMEM((512, 512), F32),
            pltpu.VMEM((2, 64, 8, 512), F32),
            pltpu.VMEM((64, 8, 512), BF16),
            pltpu.VMEM((64, 8, 512), BF16),
            pltpu.VMEM((64, 8, 512), BF16),
            pltpu.VMEM((64, 8, 512), BF16),
            pltpu.VMEM((3, 512, 512), F32),
            pltpu.VMEM((3, 256, 512), F32),
            pltpu.VMEM((3, 3, 64, 512), F32),
            pltpu.VMEM((3, 3, 16, 512), F32),
            pltpu.VMEM((3, 3, 16, 128), F32),
            pltpu.VMEM((3, 64, 512), F32),
            pltpu.VMEM((3, 16, 512), F32),
            pltpu.VMEM((3, 16, 128), F32),
            pltpu.VMEM((4, 8, 128), F32),
            pltpu.VMEM((4, 3, 8, 128), F32),
            dma((3,)),
            dma((3,)),
            dma((3,)),
            dma((3,)),
            dma((8, 3)),
            dma((8, 3)),
            dma((4,)),
            dma((4,)),
        ],
        compiler_params=pltpu.CompilerParams(
            collective_id=0, has_side_effects=True, vmem_limit_bytes=60 * 1024 * 1024
        ),
    )(
        tile_count,
        neg_ids,
        features,
        weights,
        halo_send.reshape(1, 512),
        nbr_index.reshape(512, 16),
        edge_ends.reshape(16, 512),
    )
    return wout, stat[0, 0], pre


def solution(mesh):
    dom = ("dom",)
    in_specs = (
        P("dom", None),
        P(),
        P("dom", None, None),
        P("dom", None, None),
        P("dom"),
        P("dom", None, None),
        P("dom"),
    )
    return jax.shard_map(
        on_device,
        mesh=mesh,
        in_specs=in_specs,
        out_specs=(P(), P(), P("dom", None)),
        check_vma=False,
    )
```
